8 devices in a mesh: dp: 1 (over z), sp: 8 (over y, x, core).
Axes of the slice: x: 2, y: 2, z: 1, core: 2. Of those that a mesh axis runs over, the one named last changes fastest.
Arguments:
- spec_tok: bfloat16 [64, 5, 1536], P('dp')
- patch_tok: bfloat16 [64, 256, 1536], P('dp', 'sp')
- norm1_w: bfloat16 [1536], replicated
- norm1_b: bfloat16 [1536], replicated
- w_qkv: bfloat16 [1536, 4608], replicated
- b_qkv: bfloat16 [4608], replicated
- w_out: bfloat16 [24, 64, 1536], replicated
- b_out: bfloat16 [1536], replicated
- scale_attn: bfloat16 [1536], replicated
- norm2_w: bfloat16 [1536], replicated
- norm2_b: bfloat16 [1536], replicated
- w_gate: bfloat16 [1536, 4096], replicated
- b_gate: bfloat16 [4096], replicated
- w_up: bfloat16 [1536, 4096], replicated
- b_up: bfloat16 [4096], replicated
- w_down: bfloat16 [4096, 1536], replicated
- b_down: bfloat16 [1536], replicated
- scale_mlp: bfloat16 [1536], replicated
- dy_spec: bfloat16 [64, 5, 1536], P('dp')
- dy_patch: bfloat16 [64, 256, 1536], P('dp', 'sp')
Outputs:
- output 1: bfloat16 [64, 5, 1536], P('dp')
- output 2: bfloat16 [64, 256, 1536], P('dp', 'sp')
- output 3: bfloat16 [64, 5, 1536], P('dp')
- output 4: bfloat16 [64, 256, 1536], P('dp', 'sp')
- output 5: float32 [1536], P('dp')
- output 6: float32 [1536], P('dp')
- output 7: float32 [1536, 4608], P('dp')
- output 8: float32 [4608], P('dp')
- output 9: float32 [24, 64, 1536], P('dp')
- output 10: float32 [1536], P('dp')
- output 11: float32 [1536], P('dp')
- output 12: float32 [1536], P('dp')
- output 13: float32 [1536], P('dp')
- output 14: float32 [1536, 4096], P('dp')
- output 15: float32 [4096], P('dp')
- output 16: float32 [1536, 4096], P('dp')
- output 17: float32 [4096], P('dp')
- output 18: float32 [4096, 1536], P('dp')
- output 19: float32 [1536], P('dp')
- output 20: float32 [1536], P('dp')
All inputs are finite; a program needn't handle non-finite values.
Results may differ from the reference program's by a relative error of at most 0.0173021.
Values are sent between devices in bfloat16 or wider.
A program may use at most 1 GiB of HBM per device.

```python
import jax
import jax.numpy as jnp
from jax import lax

D = 1536
HEADS = 24
HEAD = 64
FF = 4096
BATCH = 64
PATCH = 256
SPECIAL = 5
TOKENS = SPECIAL + PATCH


def draw_normal(rng_key, shape, scale):
    return (jax.random.normal(rng_key, shape, jnp.float32) * scale).astype(jnp.bfloat16)


def setup_inputs(seed: int = 0, part: int = 0) -> dict:
    base_key = jax.random.key(seed)
    data_keys = jax.random.split(jax.random.fold_in(base_key, part), 4)
    param_keys = jax.random.split(base_key, 16)

    def norm_gain(rng_key):
        return (1.0 + 0.2 * jax.random.normal(rng_key, (D,), jnp.float32)).astype(jnp.bfloat16)

    def layer_scale(rng_key):
        return jax.random.uniform(rng_key, (D,), jnp.float32, 0.3, 0.8).astype(jnp.bfloat16)

    return {
        "spec_tok": draw_normal(data_keys[0], (BATCH, SPECIAL, D), 1.0),
        "patch_tok": draw_normal(data_keys[1], (BATCH, PATCH, D), 1.0),
        "norm1_w": norm_gain(param_keys[0]),
        "norm1_b": draw_normal(param_keys[1], (D,), 0.2),
        "w_qkv": draw_normal(param_keys[2], (D, 3 * D), 1.4 * D ** -0.5),
        "b_qkv": draw_normal(param_keys[3], (3 * D,), 0.3),
        "w_out": draw_normal(param_keys[4], (HEADS, HEAD, D), D ** -0.5),
        "b_out": draw_normal(param_keys[5], (D,), 0.3),
        "scale_attn": layer_scale(param_keys[6]),
        "norm2_w": norm_gain(param_keys[7]),
        "norm2_b": draw_normal(param_keys[8], (D,), 0.2),
        "w_gate": draw_normal(param_keys[9], (D, FF), D ** -0.5),
        "b_gate": draw_normal(param_keys[10], (FF,), 0.3),
        "w_up": draw_normal(param_keys[11], (D, FF), D ** -0.5),
        "b_up": draw_normal(param_keys[12], (FF,), 0.3),
        "w_down": draw_normal(param_keys[13], (FF, D), FF ** -0.5),
        "b_down": draw_normal(param_keys[14], (D,), 0.3),
        "scale_mlp": layer_scale(param_keys[15]),
        "dy_spec": draw_normal(data_keys[2], (BATCH, SPECIAL, D), 1.0),
        "dy_patch": draw_normal(data_keys[3], (BATCH, PATCH, D), 1.0),
    }


def to_bf(values):
    return values.astype(jnp.bfloat16).astype(jnp.float32)


def layer_norm(tokens, weight, bias):
    row_mean = jnp.mean(tokens, axis=-1, keepdims=True)
    centred = tokens - row_mean
    row_var = jnp.mean(centred * centred, axis=-1, keepdims=True)
    return centred * lax.rsqrt(row_var + 1e-6) * weight + bias


def one_head(head_qkv):
    scores = jnp.einsum("bqd,bkd->bqk", head_qkv[0], head_qkv[1]) * HEAD ** -0.5
    attn_probs = to_bf(jax.nn.softmax(scores, axis=-1))
    return to_bf(jnp.einsum("bqk,bkd->bqd", attn_probs, head_qkv[2]))


def block_forward(tokens, params):
    (norm1_w, norm1_b, w_qkv, b_qkv, w_out, b_out, scale_attn, norm2_w, norm2_b,
     w_gate, b_gate, w_up, b_up, w_down, b_down, scale_mlp) = params
    normed1 = to_bf(layer_norm(tokens, norm1_w, norm1_b))
    qkv_all = to_bf(jnp.einsum("btd,de->bte", normed1, w_qkv) + b_qkv)
    heads_first = qkv_all.reshape(BATCH, TOKENS, 3, HEADS, HEAD).transpose(3, 2, 0, 1, 4)
    context = lax.map(jax.checkpoint(one_head), heads_first)
    branch1 = jnp.einsum("hbtd,hde->bte", context, w_out) + b_out
    resid_tok = to_bf(tokens + scale_attn * branch1)
    normed2 = to_bf(layer_norm(resid_tok, norm2_w, norm2_b))
    gate_pre = jnp.einsum("btd,df->btf", normed2, w_gate) + b_gate
    up_proj = jnp.einsum("btd,df->btf", normed2, w_up) + b_up
    hidden = to_bf(jax.nn.silu(gate_pre) * up_proj)
    branch2 = jnp.einsum("btf,fd->btd", hidden, w_down) + b_down
    return to_bf(resid_tok + scale_mlp * branch2)


def reference(spec_tok, patch_tok, norm1_w, norm1_b, w_qkv, b_qkv, w_out, b_out, scale_attn,
              norm2_w, norm2_b, w_gate, b_gate, w_up, b_up, w_down, b_down, scale_mlp,
              dy_spec, dy_patch):
    params = tuple(param_arr.astype(jnp.float32) for param_arr in (
        norm1_w, norm1_b, w_qkv, b_qkv, w_out, b_out, scale_attn, norm2_w, norm2_b,
        w_gate, b_gate, w_up, b_up, w_down, b_down, scale_mlp))
    tokens = jnp.concatenate([spec_tok, patch_tok], axis=1).astype(jnp.float32)
    block_out, pullback = jax.vjp(block_forward, tokens, params)
    d_out = jnp.concatenate([dy_spec, dy_patch], axis=1).astype(jnp.float32)
    d_tokens, d_params = pullback(d_out)
    (g_norm1_w, g_norm1_b, g_w_qkv, g_b_qkv, g_w_out, g_b_out, g_scale_attn, g_norm2_w, g_norm2_b,
     g_w_gate, g_b_gate, g_w_up, g_b_up, g_w_down, g_b_down, g_scale_mlp) = d_params
    out_half = block_out.astype(jnp.bfloat16)
    grad_half = d_tokens.astype(jnp.bfloat16)
    return (out_half[:, :SPECIAL], out_half[:, SPECIAL:], grad_half[:, :SPECIAL], grad_half[:, SPECIAL:],
            g_norm1_w, g_norm1_b, g_w_qkv, g_b_qkv, g_w_out, g_b_out, g_scale_attn, g_norm2_w, g_norm2_b,
            g_w_gate, g_b_gate, g_w_up, g_b_up, g_w_down, g_b_down, g_scale_mlp)
```

```python
import functools

import jax
import jax.numpy as jnp
from jax import lax
from jax.experimental import pallas as pl
from jax.experimental.pallas import tpu as pltpu
from jax.sharding import PartitionSpec as P

NORM_EPS = 1e-6
SPECIAL = 5
PAD_SPECIAL = 8
LANES = 128
F32 = jnp.float32
BF16 = jnp.bfloat16


def norm_forward(tok_f32, weight, bias):
    row_mean = jnp.mean(tok_f32, axis=-1, keepdims=True)
    centred = tok_f32 - row_mean
    inv_std = lax.rsqrt(jnp.mean(centred * centred, axis=-1, keepdims=True) + NORM_EPS)
    norm_hat = centred * inv_std
    normed = (norm_hat * weight.astype(F32) + bias.astype(F32)).astype(BF16)
    return norm_hat, inv_std, normed


def norm_backward(d_normed, norm_hat, inv_std, weight):
    d_hat = d_normed * weight.astype(F32)
    mean_grad = jnp.mean(d_hat, axis=-1, keepdims=True)
    mean_proj = jnp.mean(d_hat * norm_hat, axis=-1, keepdims=True)
    return inv_std * (d_hat - mean_grad - norm_hat * mean_proj)


def dot(lhs, rhs, lhs_dim, rhs_dim):
    return lax.dot_general(lhs, rhs, (((lhs_dim,), (rhs_dim,)), ((), ())), preferred_element_type=F32)


def softmax_rows(scores, real_keys, scale):
    col = lax.broadcasted_iota(jnp.int32, scores.shape, 1)
    scores = jnp.where(col < real_keys, scores, -jnp.inf)
    row_max = jnp.max(scores, axis=1, keepdims=True)
    weights = jnp.exp((scores - row_max) * scale)
    return weights / jnp.sum(weights, axis=1, keepdims=True)


def pair_slices(ref, pair, model_width):
    return [ref[0, :, pl.ds(pl.multiple_of(part * model_width + pair * LANES, LANES), LANES)] for part in range(3)]


def attn_fwd_kernel(real_keys, head_dim, qkv_ref, ctx_ref):
    model_width = ctx_ref.shape[2]
    scale = head_dim ** -0.5

    def body(pair, carry):
        q_two, k_two, v_two = pair_slices(qkv_ref, pair, model_width)
        low = lax.broadcasted_iota(jnp.int32, q_two.shape, 1) < head_dim
        zero = jnp.zeros_like(q_two)
        parts = []
        for half in range(2):
            q_one = jnp.where(low, q_two, zero) if half == 0 else jnp.where(low, zero, q_two)
            probs = softmax_rows(dot(q_one, k_two, 1, 1), real_keys, scale).astype(BF16)
            parts.append(dot(probs, v_two, 1, 0))
        col = pl.multiple_of(pair * LANES, LANES)
        ctx_ref[0, :, pl.ds(col, LANES)] = jnp.where(low, parts[0], parts[1]).astype(BF16)
        return carry

    lax.fori_loop(0, model_width // LANES, body, 0)


def attn_bwd_kernel(real_keys, head_dim, qkv_ref, dctx_ref, dqkv_ref):
    model_width = dctx_ref.shape[2]
    scale = head_dim ** -0.5

    def body(pair, carry):
        q_two, k_two, v_two = pair_slices(qkv_ref, pair, model_width)
        col = pl.multiple_of(pair * LANES, LANES)
        do_two = dctx_ref[0, :, pl.ds(col, LANES)]
        low = lax.broadcasted_iota(jnp.int32, q_two.shape, 1) < head_dim
        zero = jnp.zeros_like(q_two)
        dq, dk, dv = [], [], []
        for half in range(2):
            q_one = jnp.where(low, q_two, zero) if half == 0 else jnp.where(low, zero, q_two)
            do_one = jnp.where(low, do_two, zero) if half == 0 else jnp.where(low, zero, do_two)
            probs = softmax_rows(dot(q_one, k_two, 1, 1), real_keys, scale)
            d_probs = dot(do_one, v_two, 1, 1)
            inner = jnp.sum(d_probs * probs, axis=1, keepdims=True)
            d_scores = (probs * (d_probs - inner) * scale).astype(BF16)
            dv.append(dot(probs.astype(BF16), do_two, 0, 0))
            dq.append(dot(d_scores, k_two, 1, 0))
            dk.append(dot(d_scores, q_two, 0, 0))
        for part, pieces in enumerate((dq, dk, dv)):
            start = pl.multiple_of(part * model_width + pair * LANES, LANES)
            dqkv_ref[0, :, pl.ds(start, LANES)] = jnp.where(low, pieces[0], pieces[1]).astype(BF16)
        return carry

    lax.fori_loop(0, model_width // LANES, body, 0)


def row_block(rows, width):
    return pl.BlockSpec((1, rows, width), lambda image: (image, 0, 0))


def attn_cost(images, rows, width, head_dim, products):
    heads = width // head_dim
    return pl.CostEstimate(flops=2 * products * images * heads * rows * rows * 4 * head_dim,
                           bytes_accessed=images * rows * width * 2 * (4 if products == 2 else 7),
                           transcendentals=images * heads * rows * rows)


def attn_forward(qkv, real_keys, head_dim):
    images, rows, width3 = qkv.shape
    width = width3 // 3
    return pl.pallas_call(
        functools.partial(attn_fwd_kernel, real_keys, head_dim),
        out_shape=jax.ShapeDtypeStruct((images, rows, width), BF16),
        grid=(images,),
        in_specs=[row_block(rows, width3)],
        out_specs=row_block(rows, width),
        compiler_params=pltpu.CompilerParams(vmem_limit_bytes=60 * 2**20),
        cost_estimate=attn_cost(images, rows, width, head_dim, 2),
        name="attn_fwd",
    )(qkv)


def attn_backward(qkv, d_ctx, real_keys, head_dim):
    images, rows, width3 = qkv.shape
    width = width3 // 3
    return pl.pallas_call(
        functools.partial(attn_bwd_kernel, real_keys, head_dim),
        out_shape=jax.ShapeDtypeStruct((images, rows, width3), BF16),
        grid=(images,),
        in_specs=[row_block(rows, width3), row_block(rows, width)],
        out_specs=row_block(rows, width3),
        compiler_params=pltpu.CompilerParams(vmem_limit_bytes=60 * 2**20),
        cost_estimate=attn_cost(images, rows, width, head_dim, 5),
        name="attn_bwd",
    )(qkv, d_ctx)


def solution(mesh):
    groups = mesh.shape["sp"]
    tok_spec = P("dp", None, None)
    seq_spec = P("dp", "sp", None)
    shared = P()
    vec_spec = P("dp")
    mat_spec = P("dp", None)

    def local_block(spec_tok, patch_tok, norm1_w, norm1_b, w_qkv, b_qkv, w_out, b_out, scale_attn,
                    norm2_w, norm2_b, w_gate, b_gate, w_up, b_up, w_down, b_down, scale_mlp,
                    dy_spec, dy_patch):
        num_heads, head_dim, width = w_out.shape
        batch, local_patch = patch_tok.shape[0], patch_tok.shape[1]
        images = batch // groups
        patches = groups * local_patch
        rows = patches + PAD_SPECIAL
        real_rows = patches + SPECIAL
        total = images * rows
        rank = lax.axis_index("sp")

        def to_images(special, patch):
            sent = patch.reshape(groups, images, local_patch, width)
            got = lax.all_to_all(sent, "sp", 0, 0, tiled=True)
            got = jnp.transpose(got, (1, 0, 2, 3)).reshape(images, patches, width)
            own = lax.dynamic_slice_in_dim(special, rank * images, images, axis=0)
            own = jnp.pad(own, ((0, 0), (0, PAD_SPECIAL - SPECIAL), (0, 0)))
            return jnp.concatenate([got, own], axis=1).reshape(total, width)

        def from_images(value):
            value = value.reshape(images, rows, width)
            sent = jnp.transpose(value[:, :patches].reshape(images, groups, local_patch, width), (1, 0, 2, 3))
            patch = lax.all_to_all(sent, "sp", 0, 0, tiled=True).reshape(batch, local_patch, width)
            special = lax.all_gather(value[:, patches:real_rows], "sp", axis=0, tiled=True)
            return special, patch

        def col_sum(value):
            return jnp.sum(value, axis=0)

        tok_f32 = to_images(spec_tok, patch_tok).astype(F32)
        d_out = to_images(dy_spec, dy_patch).astype(F32)
        norm_hat1, inv_std1, normed1 = norm_forward(tok_f32, norm1_w, norm1_b)
        qkv = (dot(normed1, w_qkv, 1, 0) + b_qkv.astype(F32)).astype(BF16)
        qkv3 = qkv.reshape(images, rows, 3 * width)
        ctx = attn_forward(qkv3, real_rows, head_dim).reshape(total, width)
        w_out2 = w_out.reshape(width, width)
        branch1 = dot(ctx, w_out2, 1, 0) + b_out.astype(F32)
        resid_f32 = (tok_f32 + scale_attn.astype(F32) * branch1).astype(BF16).astype(F32)
        norm_hat2, inv_std2, normed2 = norm_forward(resid_f32, norm2_w, norm2_b)
        gate_pre = dot(normed2, w_gate, 1, 0) + b_gate.astype(F32)
        up_proj = dot(normed2, w_up, 1, 0) + b_up.astype(F32)
        gate_sig = jax.nn.sigmoid(gate_pre)
        gate_act = gate_pre * gate_sig
        hidden = (gate_act * up_proj).astype(BF16)
        branch2 = dot(hidden, w_down, 1, 0) + b_down.astype(F32)
        block_out = (resid_f32 + scale_mlp.astype(F32) * branch2).astype(BF16)

        g_scale_mlp = col_sum(d_out * branch2)
        d_branch2 = d_out * scale_mlp.astype(F32)
        g_b_down = col_sum(d_branch2)
        d_branch2_h = d_branch2.astype(BF16)
        g_w_down = dot(hidden, d_branch2_h, 0, 0)
        d_hidden = dot(d_branch2_h, w_down, 1, 1)
        d_up = d_hidden * gate_act
        d_gate = d_hidden * up_proj * gate_sig * (1.0 + gate_pre * (1.0 - gate_sig))
        g_b_gate = col_sum(d_gate)
        g_b_up = col_sum(d_up)
        d_gate_h = d_gate.astype(BF16)
        d_up_h = d_up.astype(BF16)
        g_w_gate = dot(normed2, d_gate_h, 0, 0)
        g_w_up = dot(normed2, d_up_h, 0, 0)
        d_normed2 = dot(d_gate_h, w_gate, 1, 1) + dot(d_up_h, w_up, 1, 1)
        g_norm2_w = col_sum(d_normed2 * norm_hat2)
        g_norm2_b = col_sum(d_normed2)
        d_resid = d_out + norm_backward(d_normed2, norm_hat2, inv_std2, norm2_w)
        g_scale_attn = col_sum(d_resid * branch1)
        d_branch1 = d_resid * scale_attn.astype(F32)
        g_b_out = col_sum(d_branch1)
        d_branch1_h = d_branch1.astype(BF16)
        g_w_out = dot(ctx, d_branch1_h, 0, 0).reshape(num_heads, head_dim, width)
        d_ctx = dot(d_branch1_h, w_out2, 1, 1).astype(BF16)
        d_qkv = attn_backward(qkv3, d_ctx.reshape(images, rows, width), real_rows, head_dim).reshape(total, 3 * width)
        g_b_qkv = col_sum(d_qkv.astype(F32))
        g_w_qkv = dot(normed1, d_qkv, 0, 0)
        d_normed1 = dot(d_qkv, w_qkv, 1, 1)
        g_norm1_w = col_sum(d_normed1 * norm_hat1)
        g_norm1_b = col_sum(d_normed1)
        d_tokens = (d_resid + norm_backward(d_normed1, norm_hat1, inv_std1, norm1_w)).astype(BF16)
        out_spec, out_patch = from_images(block_out)
        grad_spec, grad_patch = from_images(d_tokens)
        all_grads = lax.psum((g_norm1_w, g_norm1_b, g_w_qkv, g_b_qkv, g_w_out, g_b_out, g_scale_attn,
                              g_norm2_w, g_norm2_b, g_w_gate, g_b_gate, g_w_up, g_b_up, g_w_down, g_b_down,
                              g_scale_mlp), "sp")
        return (out_spec, out_patch, grad_spec, grad_patch) + all_grads

    in_specs = (tok_spec, seq_spec) + (shared,) * 16 + (tok_spec, seq_spec)
    out_specs = (tok_spec, seq_spec, tok_spec, seq_spec, vec_spec, vec_spec, mat_spec, vec_spec,
                 P("dp", None, None), vec_spec, vec_spec, vec_spec, vec_spec, mat_spec, vec_spec,
                 mat_spec, vec_spec, mat_spec, vec_spec, vec_spec)
    return jax.shard_map(local_block, mesh=mesh, in_specs=in_specs, out_specs=out_specs, check_vma=False)
```
